256 devices in a mesh: row: 16 (over x, y), col: 16 (over z, core).
Axes of the slice: x: 4, y: 4, z: 8, core: 2. Of those that a mesh axis runs over, the one named last changes fastest.
Arguments:
- values: bfloat16 [8192, 8192], P('row', 'col'), may hold values from 0.0001296997 to 0.12988281
- tile_mask: int32 [64, 64], P('row', 'col'), may hold values 0 or 1
- keep_mask: int32 [64, 64], P('row', 'col'), may hold values 0 or 1
- thr_index: int32 [8192], P('col'), may hold values from 0 to 9
Outputs:
- expanded: bfloat16 [8192, 8192], P('row', 'col')
The draws below stay inside these ranges and needn't reach their ends.
All inputs are finite; a program needn't handle non-finite values. No bound on the sum of `tile_mask` or of `keep_mask` on one device may be relied on, other than what follows from the above.
Results may differ from the reference program's by a relative error of at most 0.0004.
Values may be sent and summed in bfloat16 or wider, within the bound.
No kernel may reach another device: no remote copies, remote signals or barrier semaphores. Data moves between devices by JAX's collectives and lax.ppermute only.
A program may use at most 64 MiB of HBM per device.

```python
import math
import jax
import jax.numpy as jnp

TB = 128
NT = 64
ORDER = 8192


def touch_ends(values, stream_key, smallest, largest):
    spot = [jax.random.randint(jax.random.fold_in(stream_key, axis), (), 0, length) for axis, length in enumerate(values.shape)]
    longest = values.shape.index(max(values.shape))
    neighbour = spot[:longest] + [(spot[longest] + 1) % values.shape[longest]] + spot[longest + 1:]
    return values.at[tuple(spot)].set(smallest).at[tuple(neighbour)].set(largest)


def levels(stream_key, extent, shards, least, largest):
    level = 1.0
    for dim, shards_of in shards:
        draws = jax.random.uniform(jax.random.fold_in(jax.random.fold_in(stream_key, 6), dim), (shards_of,), jnp.float32, least / len(shards), largest / len(shards))
        level = level * jnp.repeat(jnp.exp(draws), extent[dim] // shards_of).reshape((-1,) + (1,) * (len(extent) - 1 - dim))
    return level


def setup_inputs(seed: int = 0) -> dict:
    seeds = jax.random.split(jax.random.key(seed), 5)
    values = jnp.clip(jnp.exp(math.log(0.12988281) - 6.909166 * jax.random.uniform(seeds[0], (ORDER, ORDER), jnp.float32) ** levels(seeds[0], (ORDER, ORDER), ((0, 16), (1, 16)), -0.2, 0.2)), 0.0001296997, 0.12988281).astype(jnp.bfloat16)
    tile_mask = touch_ends((jax.random.randint(seeds[1], (NT, NT), 0, 2) < 1).astype(jnp.int32), jax.random.fold_in(seeds[1], 1), 0, 1)
    keep_mask = touch_ends((jax.random.randint(seeds[2], (NT, NT), 0, 4) < 3).astype(jnp.int32), jax.random.fold_in(seeds[2], 1), 0, 1)
    thr_index = touch_ends(jax.random.randint(seeds[3], (ORDER,), 0, 10), jax.random.fold_in(seeds[3], 1), 0, 9).astype(jnp.int32)
    return {"values": values, "tile_mask": tile_mask, "keep_mask": keep_mask, "thr_index": thr_index}


def reference(values, tile_mask, keep_mask, thr_index):
    matrix = (values.reshape(NT, TB, NT, TB) * tile_mask[:, None, :, None].astype(jnp.bfloat16)).reshape(ORDER, ORDER)
    product = jnp.dot(matrix, matrix, preferred_element_type=jnp.float32)
    col_means = jnp.sum(product, axis=0) / ORDER
    thresholds = 0.125 * thr_index.astype(jnp.float32)
    kept_cells = jnp.broadcast_to(keep_mask[:, None, :, None].astype(jnp.float32), (NT, TB, NT, TB)).reshape(ORDER, ORDER)
    pruned = jnp.maximum(product - thresholds * col_means, 0.0) * kept_cells
    col_totals = jnp.sum(pruned, axis=0) / ORDER
    return (pruned / jnp.maximum(col_totals, 0.1)).astype(jnp.bfloat16)
```

```python
import jax
import jax.numpy as jnp
from jax import lax
from jax.sharding import Mesh
from jax.sharding import PartitionSpec as P

TB = 128
NX, NY, NZ, NC = 4, 4, 8, 2
ROW = ("x", "y")
COL = ("z", "c")

XYC = [(x, y, c) for x in range(NX) for y in range(NY) for c in range(NC)]


def xyc(x, y, c):
    return ((x % NX) * NY + y % NY) * NC + c


def along_first(block, step):
    pairs = [(xyc(x, y, c), xyc(x + step, y, c) if c == 0 else xyc(x, y + step, c)) for x, y, c in XYC]
    return lax.ppermute(block, ("x", "y", "c"), pairs)


def along_second(block, step):
    pairs = [(xyc(x, y, c), xyc(x, y + step, c) if c == 0 else xyc(x + step, y, c)) for x, y, c in XYC]
    return lax.ppermute(block, ("x", "y", "c"), pairs)


def ring_z(block):
    pairs = [
        (z * NC + c, ((z + 1 - 2 * c) % NZ) * NC + c) for z in range(NZ) for c in range(NC)
    ]
    return lax.ppermute(block, ("z", "c"), pairs)


def partner(block):
    return lax.ppermute(block, "c", [(0, 1), (1, 0)])


def sum_over_rows(part):
    spread = jnp.broadcast_to(part[None, :], (NX * NY, part.shape[0]))
    return jnp.sum(lax.all_to_all(spread, ROW, 0, 0, tiled=True), axis=0)


def on_device(values, tile_mask, keep_mask, thr_index):
    n = values.shape[0]
    tiles = n // TB
    x, y, z, c = (lax.axis_index(a) for a in ("x", "y", "z", "c"))
    first = jnp.where(c == 0, x, y)
    second = jnp.where(c == 0, y, x)

    def expand(mask, dtype):
        return jnp.broadcast_to(
            mask[:, None, :, None].astype(dtype), (tiles, TB, tiles, TB)
        ).reshape(n, n)

    own = values * expand(tile_mask, jnp.bfloat16)
    order_all = n * NX * NY

    cols = {(0, 0): own}
    cols[1, 0] = along_first(own, 1)
    cols[3, 0] = along_first(own, -1)
    cols[2, 0] = along_first(own, 2)
    for j in (0, 1, 3, 2):
        cols[j, 1] = along_second(cols[j, 0], 1)
        cols[j, 3] = along_second(cols[j, 0], -1)
    for j in (0, 1):
        cols[j, 2] = along_second(cols[j, 1], 1)
    for j in (3, 2):
        cols[j, 2] = along_second(cols[j, 3], -1)

    other = partner(own)
    rows = [(z, c, own), (z, 1 - c, other)]
    a, b = own, other
    back = 1 - 2 * c
    for step in range(1, NZ // 2 + 1):
        a = ring_z(a)
        rows.append((z - back * step, c, a))
        rows.append((z + back * step, 1 - c, partner(a)))
        if step < NZ // 2:
            b = ring_z(b)
            rows.append((z - back * step, 1 - c, b))
            rows.append((z + back * step, c, partner(b)))

    row_panel = jnp.zeros((n, n * NZ * NC), jnp.bfloat16)
    for zz, cc, block in rows:
        at = (zz % NZ) * NC + cc
        row_panel = lax.dynamic_update_slice(row_panel, block, (0, at * n))
    col_panel = jnp.zeros((order_all, n), jnp.bfloat16)
    for (j, i), block in cols.items():
        p, q = (first - j) % 4, (second - i) % 4
        at = jnp.where(c == 0, p * NY + q, q * NY + p)
        col_panel = lax.dynamic_update_slice(col_panel, block, (at * n, 0))

    product = jnp.dot(row_panel, col_panel, preferred_element_type=jnp.float32)
    thresholds = 0.125 * thr_index.astype(jnp.float32)
    col_means = sum_over_rows(jnp.sum(product, axis=0)) / order_all
    pruned = jnp.maximum(product - thresholds * col_means, 0.0) * expand(keep_mask, jnp.float32)
    col_totals = sum_over_rows(jnp.sum(pruned, axis=0)) / order_all
    return (pruned / jnp.maximum(col_totals, 0.1)).astype(jnp.bfloat16)


def solution(mesh):
    finer = Mesh(mesh.devices.reshape(NX, NY, NZ, NC), ("x", "y", "z", "c"))
    placed = (P(ROW, COL), P(ROW, COL), P(ROW, COL), P(COL))
    return jax.shard_map(
        on_device, mesh=finer, in_specs=placed, out_specs=P(ROW, COL), check_vma=False
    )
```

```python
import functools

import jax
import jax.numpy as jnp
from jax import lax
from jax.experimental import pallas as pl
from jax.experimental.pallas import tpu as pltpu
from jax.sharding import Mesh
from jax.sharding import PartitionSpec as P

TB = 128
NX, NY, NZ, NC = 4, 4, 8, 2
ROW = ("x", "y")
COL = ("z", "c")

XYC = [(x, y, c) for x in range(NX) for y in range(NY) for c in range(NC)]
VMEM = pl.BlockSpec(memory_space=pltpu.VMEM)
SMEM = pl.BlockSpec(memory_space=pltpu.SMEM)


def xyc(x, y, c):
    return ((x % NX) * NY + y % NY) * NC + c


def along_first(block, step):
    pairs = [(xyc(x, y, c), xyc(x + step, y, c) if c == 0 else xyc(x, y + step, c)) for x, y, c in XYC]
    return lax.ppermute(block, ("x", "y", "c"), pairs)


def along_second(block, step):
    pairs = [(xyc(x, y, c), xyc(x, y + step, c) if c == 0 else xyc(x + step, y, c)) for x, y, c in XYC]
    return lax.ppermute(block, ("x", "y", "c"), pairs)


def ring_z(block):
    pairs = [
        (z * NC + c, ((z + 1 - 2 * c) % NZ) * NC + c) for z in range(NZ) for c in range(NC)
    ]
    return lax.ppermute(block, ("z", "c"), pairs)


def partner(block):
    return lax.ppermute(block, "c", [(0, 1), (1, 0)])


def sum_over_rows(part):
    spread = jnp.broadcast_to(part[None, :], (NX * NY, part.shape[0]))
    return jnp.sum(lax.all_to_all(spread, ROW, 0, 0, tiled=True), axis=0)


def mask_kernel(mask_ref, values_ref, out_ref):
    tiles = out_ref.shape[0] // TB
    for i in range(tiles):
        for j in range(tiles):
            at = (slice(i * TB, (i + 1) * TB), slice(j * TB, (j + 1) * TB))
            keep = mask_ref[i, j].astype(jnp.float32)
            out_ref[at] = (values_ref[at].astype(jnp.float32) * keep).astype(out_ref.dtype)


def matmul_kernel(n_cols, has_acc, at_ref, rows_ref, *refs):
    col_refs, refs = refs[:n_cols], refs[n_cols:]
    n = rows_ref.shape[1]
    half = n // 2

    def body(m, carry):
        band = pl.ds(pl.multiple_of(m * half, half), half)
        total = refs[0][band, :] if has_acc else None
        for j in range(n_cols):
            part = jnp.dot(
                rows_ref[at_ref[j], band, :], col_refs[j][...], preferred_element_type=jnp.float32
            )
            total = part if total is None else total + part
        refs[-1][band, :] = total
        return carry

    lax.fori_loop(0, 2, body, 0)


def matmul(at, rows, cols, acc=None):
    n = rows.shape[1]
    args = (at, rows, *cols) + (() if acc is None else (acc,))
    return pl.pallas_call(
        functools.partial(matmul_kernel, len(cols), acc is not None),
        out_shape=jax.ShapeDtypeStruct((n, n), jnp.float32),
        in_specs=[SMEM] + [VMEM] * (len(args) - 1),
        out_specs=VMEM,
        input_output_aliases={} if acc is None else {len(args) - 1: 0},
        cost_estimate=pl.CostEstimate(
            flops=2 * n * n * n * len(cols), bytes_accessed=0, transcendentals=0
        ),
        name="matmul_first" if acc is None else "matmul_last",
    )(*args)


def on_device(values, tile_mask, keep_mask, thr_index):
    n = values.shape[0]
    tiles = n // TB
    x, y, z, c = (lax.axis_index(a) for a in ("x", "y", "z", "c"))
    first = jnp.where(c == 0, x, y)
    second = jnp.where(c == 0, y, x)
    order_all = n * NX * NY

    own = pl.pallas_call(
        mask_kernel,
        out_shape=jax.ShapeDtypeStruct((n, n), values.dtype),
        in_specs=[SMEM, VMEM],
        out_specs=VMEM,
        name="mask",
    )(tile_mask, values)

    n1 = along_first(own, 1)
    n3 = along_first(own, -1)
    other = partner(own)
    a1 = ring_z(own)
    up_o = along_second(own, 1)
    dn_o = along_second(own, -1)
    n2 = along_first(own, 2)
    b1 = ring_z(other)
    pair = jnp.stack([n1, n3])
    up_pair = along_second(pair, 1)
    dn_pair = along_second(pair, -1)
    a2 = ring_z(a1)
    b2 = ring_z(b1)
    far_o = along_second(up_o, 1)
    up_n2 = along_second(n2, 1)
    dn_n2 = along_second(n2, -1)
    far_n1 = along_second(up_pair[0], 1)
    far_n3 = along_second(dn_pair[1], -1)
    far_n2 = along_second(dn_n2, -1)
    a3 = ring_z(a2)
    b3 = ring_z(b2)
    a4 = ring_z(a3)
    d1 = partner(jnp.stack([a1, b1]))
    d2 = partner(jnp.stack([a2, b2]))
    d3 = partner(jnp.stack([a3, b3, a4]))

    early = [
        (0, 0, own), (1, 0, n1), (3, 0, n3), (2, 0, n2),
        (0, 1, up_o), (1, 1, up_pair[0]), (3, 1, up_pair[1]), (2, 1, up_n2),
        (0, 3, dn_o), (1, 3, dn_pair[0]), (3, 3, dn_pair[1]), (2, 3, dn_n2),
    ]
    late = [(0, 2, far_o), (1, 2, far_n1), (3, 2, far_n3), (2, 2, far_n2)]

    def places(blocks):
        out = []
        for j, i, _ in blocks:
            p, q = (first - j) % 4, (second - i) % 4
            out.append(jnp.where(c == 0, p * NY + q, q * NY + p))
        return jnp.stack(out).astype(jnp.int32)

    back = 1 - 2 * c
    placed = [
        (0, c, own), (0, 1 - c, other),
        (-1, c, a1), (-1, 1 - c, b1), (1, 1 - c, d1[0]), (1, c, d1[1]),
        (-2, c, a2), (-2, 1 - c, b2), (2, 1 - c, d2[0]), (2, c, d2[1]),
        (-3, c, a3), (-3, 1 - c, b3), (3, 1 - c, d3[0]), (3, c, d3[1]),
        (-4, c, a4), (4, 1 - c, d3[2]),
    ]
    rows = jnp.zeros((NZ * NC, n, n), values.dtype)
    for step, core, block in placed:
        at = ((z + back * step) % NZ) * NC + core
        rows = lax.dynamic_update_slice(rows, block[None], (at, 0, 0))

    product = matmul(places(early), rows, [b for _, _, b in early])
    product = matmul(places(late), rows, [b for _, _, b in late], product)

    def expand(mask, dtype):
        return jnp.broadcast_to(
            mask[:, None, :, None].astype(dtype), (tiles, TB, tiles, TB)
        ).reshape(n, n)

    thresholds = 0.125 * thr_index.astype(jnp.float32)
    col_means = sum_over_rows(jnp.sum(product, axis=0)) / order_all
    pruned = jnp.maximum(product - thresholds * col_means, 0.0) * expand(keep_mask, jnp.float32)
    col_totals = sum_over_rows(jnp.sum(pruned, axis=0)) / order_all
    return (pruned / jnp.maximum(col_totals, 0.1)).astype(jnp.bfloat16)


def solution(mesh):
    finer = Mesh(mesh.devices.reshape(NX, NY, NZ, NC), ("x", "y", "z", "c"))
    placed = (P(ROW, COL), P(ROW, COL), P(ROW, COL), P(COL))
    return jax.shard_map(
        on_device, mesh=finer, in_specs=placed, out_specs=P(ROW, COL), check_vma=False
    )
```

```python
import functools

import jax
import jax.numpy as jnp
from jax import lax
from jax.experimental import pallas as pl
from jax.experimental.pallas import tpu as pltpu
from jax.sharding import Mesh
from jax.sharding import PartitionSpec as P


TB = 128
EXTRA = 16
NX, NY, NZ, NC = 4, 4, 8, 2
ROW = ("x", "y")
COL = ("z", "c")

XYC = [(x, y, c) for x in range(NX) for y in range(NY) for c in range(NC)]
VMEM = pl.BlockSpec(memory_space=pltpu.VMEM)
SMEM = pl.BlockSpec(memory_space=pltpu.SMEM)


def xyc(x, y, c):
    return ((x % NX) * NY + y % NY) * NC + c


def along_first(block, step):
    pairs = [(xyc(x, y, c), xyc(x + step, y, c) if c == 0 else xyc(x, y + step, c)) for x, y, c in XYC]
    return lax.ppermute(block, ("x", "y", "c"), pairs)


def along_second(block, step):
    pairs = [(xyc(x, y, c), xyc(x, y + step, c) if c == 0 else xyc(x + step, y, c)) for x, y, c in XYC]
    return lax.ppermute(block, ("x", "y", "c"), pairs)


def ring_z(block):
    pairs = [
        (z * NC + c, ((z + 1 - 2 * c) % NZ) * NC + c) for z in range(NZ) for c in range(NC)
    ]
    return lax.ppermute(block, ("z", "c"), pairs)


def first_apart(block, apart):
    pairs = [(xyc(x, y, c), xyc(x ^ apart, y, c) if c == 0 else xyc(x, y ^ apart, c)) for x, y, c in XYC]
    return lax.ppermute(block, ("x", "y", "c"), pairs)


def against_z(block, step):
    pairs = [
        (z * NC + c, ((z - step * (1 - 2 * c)) % NZ) * NC + c) for z in range(NZ) for c in range(NC)
    ]
    return lax.ppermute(block, ("z", "c"), pairs)


def partner(block):
    return lax.ppermute(block, "c", [(0, 1), (1, 0)])


def spread_over(rows, axes):
    return lax.all_to_all(rows, axes, 0, 0, tiled=True)


def vmem(x):
    return pltpu.with_memory_space_constraint(x, pltpu.VMEM)


def local_call(kernel, out_shape, args, spaces=None, aliases=None, flops=0, limit=4, free=()):
    spaces = spaces or [VMEM] * len(args)
    args = [
        vmem(a) if s is VMEM and i not in free else a for i, (a, s) in enumerate(zip(args, spaces))
    ]
    return pl.pallas_call(
        kernel,
        out_shape=out_shape,
        in_specs=spaces,
        out_specs=jax.tree.map(lambda _: VMEM, out_shape),
        input_output_aliases=aliases or {},
        cost_estimate=pl.CostEstimate(flops=flops, bytes_accessed=0, transcendentals=0),
        compiler_params=pltpu.CompilerParams(vmem_limit_bytes=limit << 20),
    )(*args)


def mask_kernel(mask_ref, values_ref, out_ref):
    n = out_ref.shape[0]
    tiles = n // TB
    for j in range(tiles):
        for i in range(tiles):
            at = (slice(i * TB, (i + 1) * TB), slice(j * TB, (j + 1) * TB))
            keep = mask_ref[i, j].astype(jnp.float32)
            out_ref[at] = (values_ref[at].astype(jnp.float32) * keep).astype(out_ref.dtype)


def three_parts(exact):
    high = exact.astype(jnp.bfloat16).astype(jnp.float32)
    rest = exact - high
    mid = rest.astype(jnp.bfloat16).astype(jnp.float32)
    return high, mid, rest - mid


def place_sums(out_ref, sums, where):
    n = sums.shape[1]
    z, c = lax.axis_index("z"), lax.axis_index("c")
    row = lax.broadcasted_iota(jnp.int32, (EXTRA, n), 0)
    for i, (step, same) in enumerate(where):
        core = c if same else 1 - c
        at = lax.rem(z + (1 - 2 * c) * step + NZ, NZ) * NC + core
        high, mid, low = three_parts(sums[i : i + 1])
        parts = jnp.where(row == 0, high, jnp.where(row == 1, mid, jnp.where(row == 2, low, 0.0)))
        out_ref[at, pl.ds(n, EXTRA), :] = parts.astype(out_ref.dtype)


NEAR = ((0, True), (0, False), (1, True), (1, False), (-1, False), (-1, True))
AHEAD = tuple((3 + step, same) for step, same in NEAR)
BEHIND = tuple((-step, not same) for step, same in AHEAD)


def place_near_kernel(_, sums_ref, out_ref):
    place_sums(out_ref, sums_ref[...], NEAR)


def place_far_kernel(_, ahead_ref, behind_ref, out_ref):
    place_sums(out_ref, ahead_ref[...], AHEAD)
    place_sums(out_ref, behind_ref[...], BEHIND)


def far_column_kernel(own_ref, n1_ref, n3_ref, upper_ref, lower_ref, out_ref, sums_ref):
    half, n = upper_ref.shape
    total = jnp.zeros((1, n), jnp.float32)
    for ref in (own_ref, n1_ref, n3_ref, upper_ref, lower_ref):
        total += jnp.sum(ref[...].astype(jnp.float32), axis=0, keepdims=True)
    sums_ref[...] = total
    out_ref[pl.ds(0, half), :] = upper_ref[...]
    out_ref[pl.ds(half, half), :] = lower_ref[...]


def add_kernel(a_ref, b_ref, out_ref):
    out_ref[...] = a_ref[...] + b_ref[...]


def stack_kernel(*refs):
    at = 0
    for ref in refs[:-1]:
        refs[-1][pl.ds(at, ref.shape[0]), :] = ref[...]
        at += ref.shape[0]


def scale_kernel(order_all, got_ref, pruned_ref, out_ref):
    n = out_ref.shape[0]
    totals = jnp.sum(got_ref[...], axis=0, keepdims=True) / order_all
    scale = 1.0 / jnp.maximum(totals, 0.1)
    out_ref[...] = (pruned_ref[pl.ds(0, n), :] * scale).astype(out_ref.dtype)


def block_of(ref, index):
    return ref[...] if index is None else ref[index]


def pack(parts):
    def kernel(*refs):
        for i, (_, index) in enumerate(parts):
            if len(parts) == 1:
                refs[-1][...] = block_of(refs[i], index)
            else:
                refs[-1][i] = block_of(refs[i], index)

    shape = parts[0][0].shape[-2:]
    shape = shape if len(parts) == 1 else (len(parts), *shape)
    return local_call(kernel, pltpu.VMEM(shape, parts[0][0].dtype), [a for a, _ in parts])


def pick_half(block, half):
    n = block.shape[0] // 2

    def kernel(ref, out_ref):
        out_ref[...] = ref[pl.ds(half * n, n), :]

    return local_call(kernel, pltpu.VMEM((n, block.shape[1]), block.dtype), [block])


def place(stack, parts):
    def kernel(*refs):
        refs = refs if stack is None else refs[1:]
        z, c = lax.axis_index("z"), lax.axis_index("c")
        back = 1 - 2 * c
        for ref, (step, flip, _, index) in zip(refs, parts):
            core = 1 - c if flip else c
            at = lax.rem(z + back * step + NZ, NZ) * NC + core
            refs[-1][at, pl.ds(0, n), :] = block_of(ref, index)

    args = [a for _, _, a, _ in parts]
    n = args[0].shape[-1]
    out = pltpu.VMEM((NZ * NC, n + EXTRA, n), args[0].dtype)
    if stack is None:
        return local_call(kernel, out, args)
    return local_call(kernel, out, [stack, *args], aliases={0: 0})


def multiply(rows_ref, acc_ref, out_ref, parts, col_refs):
    x, y, c = (lax.axis_index(a) for a in ("x", "y", "c"))
    first = jnp.where(c == 0, x, y)
    second = jnp.where(c == 0, y, x)
    ats = []
    for j, i, _, _ in parts:
        p, q = lax.rem(first + 4 - j, 4), lax.rem(second + 4 - i, 4)
        ats.append(jnp.where(c == 0, p * NY + q, q * NY + p))
    half = out_ref.shape[1] // 2
    for band in (pl.ds(0, half), pl.ds(half, half + EXTRA)):
        total = None if acc_ref is None else acc_ref[band, :]
        for at, ref, (_, _, _, index) in zip(ats, col_refs, parts):
            part = jnp.dot(
                rows_ref[at, band, :], block_of(ref, index), preferred_element_type=jnp.float32
            )
            total = part if total is None else total + part
        out_ref[band, :] = total


def matmul_early(rows, parts):
    n = rows.shape[2]

    def kernel(rows_ref, *refs):
        multiply(rows_ref, None, refs[-1], parts, refs[:-1])

    return local_call(
        kernel,
        pltpu.VMEM((n + EXTRA, n), jnp.float32),
        [rows, *(a for _, _, a, _ in parts)],
        flops=2 * n * n * n * len(parts),
        limit=16,
    )


def matmul_late(rows, parts, product, keep_mask, thr_index, order_all):
    n = rows.shape[2]
    tiles = n // TB

    def kernel(keep_ref, thr_ref, rows_ref, *refs):
        col_refs, (acc_ref, out_ref, sums_ref) = refs[: len(parts)], refs[len(parts) :]
        multiply(rows_ref, acc_ref, out_ref, parts, col_refs)
        means = jnp.sum(out_ref[pl.ds(n, 8), :], axis=0, keepdims=True) / order_all
        cut = 0.125 * thr_ref[...].astype(jnp.float32) * means
        for j in range(tiles):
            cols = slice(j * TB, (j + 1) * TB)
            total = jnp.zeros((1, TB), jnp.float32)
            for i in range(tiles):
                at = (slice(i * TB, (i + 1) * TB), cols)
                keep = keep_ref[i, j].astype(jnp.float32)
                pruned = jnp.maximum(out_ref[at] - cut[:, cols], 0.0) * keep
                out_ref[at] = pruned
                total += jnp.sum(pruned, axis=0, keepdims=True)
            sums_ref[:, cols] = jnp.broadcast_to(total, (sums_ref.shape[0], TB))

    args = [keep_mask, thr_index, rows, *(a for _, _, a, _ in parts), product]
    return local_call(
        kernel,
        [pltpu.VMEM((n + EXTRA, n), jnp.float32), pltpu.VMEM((NX * NY, n), jnp.float32)],
        args,
        spaces=[SMEM] + [VMEM] * (len(args) - 1),
        aliases={len(args) - 1: 0},
        flops=2 * n * n * n * len(parts),
        limit=16,
    )


def expand_and_prune(values, tile_mask, keep_mask, thr_index):
    n = values.shape[0]
    order_all = n * NX * NY
    own = local_call(
        mask_kernel, pltpu.VMEM((n, n), values.dtype), [tile_mask, values], [SMEM, VMEM], free=(1,)
    )

    other = partner(own)
    n1 = along_first(own, 1)
    n3 = along_first(own, -1)
    a1 = ring_z(own)
    up_o = along_second(own, 1)
    dn_o = along_second(own, -1)
    b1 = ring_z(other)
    a2 = ring_z(a1)
    b2 = ring_z(b1)
    a3 = ring_z(a2)
    b3 = ring_z(b2)
    a4 = ring_z(a3)
    n2_upper = along_first(pick_half(n1, 0), 1)
    n2_lower = along_first(pick_half(n3, 1), -1)
    pair = pack([(n1, None), (n3, None)])
    up_pair = along_second(pair, 1)
    dn_pair = along_second(pair, -1)
    one = pltpu.VMEM((1, n), jnp.float32)
    n2, sums = local_call(
        far_column_kernel, [pltpu.VMEM((n, n), own.dtype), one], [own, n1, n3, n2_upper, n2_lower]
    )
    up_n2 = along_second(n2, 1)
    dn_n2 = along_second(n2, -1)
    far_a = along_second(pack([(up_o, None), (up_pair, 0)]), 1)
    far_b = along_second(pack([(dn_pair, 1), (dn_n2, None)]), -1)
    pairs = [(a1, None), (b1, None), (a2, None), (b2, None)]
    d1 = partner(pack(pairs))
    d3 = partner(pack([(a3, None), (b3, None)]))

    sums = partner(sums)
    sums = local_call(add_kernel, one, [sums, first_apart(sums, 1)])
    sums = local_call(add_kernel, one, [sums, first_apart(sums, 2)])
    here = local_call(stack_kernel, pltpu.VMEM((2, n), jnp.float32), [partner(sums), sums])
    next_z = against_z(here, 1)
    before = partner(next_z)
    near = local_call(stack_kernel, pltpu.VMEM((6, n), jnp.float32), [here, next_z, before])
    ahead = against_z(near, 3)
    behind = partner(ahead)
    d4 = partner(a4)

    rows = place(None, [(0, False, own, None), (0, True, other, None)])
    rows = place(rows, [(-1, False, a1, None), (-1, True, b1, None)])
    rows = place(rows, [(-2, False, a2, None), (-2, True, b2, None)])
    rows = place(rows, [(1, True, d1, 0), (1, False, d1, 1), (2, True, d1, 2), (2, False, d1, 3)])
    rows = place(rows, [(-3, False, a3, None), (-3, True, b3, None)])
    stack = pltpu.VMEM(rows.shape, rows.dtype)
    rows = place(rows, [(3, True, d3, 0), (3, False, d3, 1)])
    rows = local_call(place_near_kernel, stack, [rows, near], aliases={0: 0})
    rows = local_call(place_far_kernel, stack, [rows, ahead, behind], aliases={0: 0})
    rows = place(rows, [(4, False, a4, None), (4, True, d4, None)])

    product = matmul_early(
        rows,
        [
            (0, 0, own, None), (1, 0, n1, None), (3, 0, n3, None), (2, 0, n2, None),
            (0, 1, up_o, None), (1, 1, up_pair, 0), (3, 1, up_pair, 1), (2, 1, up_n2, None),
            (0, 3, dn_o, None), (1, 3, dn_pair, 0), (3, 3, dn_pair, 1), (2, 3, dn_n2, None),
        ],
    )
    pruned, sums = matmul_late(
        rows,
        [(0, 2, far_a, 0), (1, 2, far_a, 1), (3, 2, far_b, 0), (2, 2, far_b, 1)],
        product,
        keep_mask,
        thr_index[None, :],
        order_all,
    )
    got = spread_over(sums, ROW)
    return local_call(
        functools.partial(scale_kernel, order_all),
        jax.ShapeDtypeStruct((n, n), values.dtype),
        [got, pruned],
    )


def solution(mesh):
    finer = Mesh(mesh.devices.reshape(NX, NY, NZ, NC), ("x", "y", "z", "c"))
    placed = (P(ROW, COL), P(ROW, COL), P(ROW, COL), P(COL))
    return jax.shard_map(
        expand_and_prune, mesh=finer, in_specs=placed, out_specs=P(ROW, COL), check_vma=False
    )
```

```python
import functools

import jax
import jax.numpy as jnp
from jax import lax
from jax.experimental import pallas as pl
from jax.experimental.pallas import tpu as pltpu
from jax.sharding import Mesh
from jax.sharding import PartitionSpec as P


TB = 128
EXTRA = 16
NX, NY, NZ, NC = 4, 4, 8, 2
ROW = ("x", "y")
COL = ("z", "c")

XYC = [(x, y, c) for x in range(NX) for y in range(NY) for c in range(NC)]
VMEM = pl.BlockSpec(memory_space=pltpu.VMEM)
HBM = pl.BlockSpec(memory_space=pltpu.HBM)
SMEM = pl.BlockSpec(memory_space=pltpu.SMEM)


def xyc(x, y, c):
    return ((x % NX) * NY + y % NY) * NC + c


def along_first(block, step):
    pairs = [(xyc(x, y, c), xyc(x + step, y, c) if c == 0 else xyc(x, y + step, c)) for x, y, c in XYC]
    return lax.ppermute(block, ("x", "y", "c"), pairs)


def along_second(block, step):
    pairs = [(xyc(x, y, c), xyc(x, y + step, c) if c == 0 else xyc(x + step, y, c)) for x, y, c in XYC]
    return lax.ppermute(block, ("x", "y", "c"), pairs)


def ring_z(block):
    pairs = [
        (z * NC + c, ((z + 1 - 2 * c) % NZ) * NC + c) for z in range(NZ) for c in range(NC)
    ]
    return lax.ppermute(block, ("z", "c"), pairs)


def first_apart(block, apart):
    pairs = [(xyc(x, y, c), xyc(x ^ apart, y, c) if c == 0 else xyc(x, y ^ apart, c)) for x, y, c in XYC]
    return lax.ppermute(block, ("x", "y", "c"), pairs)


def against_z(block, step):
    pairs = [
        (z * NC + c, ((z - step * (1 - 2 * c)) % NZ) * NC + c) for z in range(NZ) for c in range(NC)
    ]
    return lax.ppermute(block, ("z", "c"), pairs)


def partner(block):
    return lax.ppermute(block, "c", [(0, 1), (1, 0)])


def spread_over(rows, axes):
    return lax.all_to_all(rows, axes, 0, 0, tiled=True)


def kept_in(x, spec):
    if spec is SMEM:
        return x
    return pltpu.with_memory_space_constraint(x, spec.memory_space)


def local_call(kernel, out_shape, args, spaces=None, aliases=None, flops=0, limit=4, scratch=()):
    spaces = spaces or [VMEM] * len(args)
    args = [kept_in(a, s) for a, s in zip(args, spaces)]
    return pl.pallas_call(
        kernel,
        out_shape=out_shape,
        in_specs=spaces,
        out_specs=jax.tree.map(lambda _: VMEM, out_shape),
        scratch_shapes=scratch,
        input_output_aliases=aliases or {},
        cost_estimate=pl.CostEstimate(flops=flops, bytes_accessed=0, transcendentals=0),
        compiler_params=pltpu.CompilerParams(vmem_limit_bytes=limit << 20),
    )(*args)


def mask_kernel(mask_hbm, values_hbm, out_ref, sums_ref, mask_ref, values_ref, sems):
    fetch_mask = pltpu.make_async_copy(mask_hbm, mask_ref, sems.at[0])
    fetch_values = pltpu.make_async_copy(values_hbm, values_ref, sems.at[1])
    fetch_mask.start()
    fetch_values.start()
    fetch_mask.wait()
    fetch_values.wait()
    tiles = out_ref.shape[0] // TB
    for j in range(tiles):
        cols = slice(j * TB, (j + 1) * TB)
        total = jnp.zeros((1, TB), jnp.float32)
        for i in range(tiles):
            at = (slice(i * TB, (i + 1) * TB), cols)
            block = values_ref[at].astype(jnp.float32) * mask_ref[i, j].astype(jnp.float32)
            out_ref[at] = block.astype(out_ref.dtype)
            total += jnp.sum(block, axis=0, keepdims=True)
        sums_ref[:, cols] = total


def join_kernel(upper_ref, lower_ref, out_ref):
    n = upper_ref.shape[0]
    out_ref[pl.ds(0, n), :] = upper_ref[...]
    out_ref[pl.ds(n, n), :] = lower_ref[...]


def three_parts(exact):
    high = exact.astype(jnp.bfloat16).astype(jnp.float32)
    rest = exact - high
    mid = rest.astype(jnp.bfloat16).astype(jnp.float32)
    return high, mid, rest - mid


def place_sums(out_ref, sums, where):
    n = sums.shape[1]
    z, c = lax.axis_index("z"), lax.axis_index("c")
    row = lax.broadcasted_iota(jnp.int32, (EXTRA, n), 0)
    for i, (step, same) in enumerate(where):
        core = c if same else 1 - c
        at = lax.rem(z + (1 - 2 * c) * step + NZ, NZ) * NC + core
        high, mid, low = three_parts(sums[i : i + 1])
        parts = jnp.where(row == 0, high, jnp.where(row == 1, mid, jnp.where(row == 2, low, 0.0)))
        out_ref[at, pl.ds(n, EXTRA), :] = parts.astype(out_ref.dtype)


NEAR = ((0, True), (0, False), (1, True), (1, False), (-1, False), (-1, True))
AHEAD = tuple((3 + step, same) for step, same in NEAR)
BEHIND = tuple((-step, not same) for step, same in AHEAD)


def place_near_kernel(_, sums_ref, out_ref):
    place_sums(out_ref, sums_ref[...], NEAR)


def place_far_kernel(_, ahead_ref, behind_ref, out_ref):
    place_sums(out_ref, ahead_ref[...], AHEAD)
    place_sums(out_ref, behind_ref[...], BEHIND)


def first_axis_kernel(mine_ref, across_ref, n1_ref, n3_ref, out_ref):
    total = mine_ref[...] + across_ref[...]
    for ref in (n1_ref, n3_ref):
        total += jnp.sum(ref[...].astype(jnp.float32), axis=0, keepdims=True)
    out_ref[...] = total


def add_kernel(a_ref, b_ref, out_ref):
    out_ref[...] = a_ref[...] + b_ref[...]


def stack_kernel(*refs):
    at = 0
    for ref in refs[:-1]:
        refs[-1][pl.ds(at, ref.shape[0]), :] = ref[...]
        at += ref.shape[0]


def scale_kernel(order_all, got_ref, pruned_ref, out_ref):
    n = out_ref.shape[0]
    totals = jnp.sum(got_ref[...], axis=0, keepdims=True) / order_all
    scale = 1.0 / jnp.maximum(totals, 0.1)
    out_ref[...] = (pruned_ref[pl.ds(0, n), :] * scale).astype(out_ref.dtype)


def block_of(ref, index):
    return ref[...] if index is None else ref[index]


def pack(parts):
    def kernel(*refs):
        for i, (_, index) in enumerate(parts):
            if len(parts) == 1:
                refs[-1][...] = block_of(refs[i], index)
            else:
                refs[-1][i] = block_of(refs[i], index)

    shape = parts[0][0].shape[-2:]
    shape = shape if len(parts) == 1 else (len(parts), *shape)
    return local_call(kernel, pltpu.VMEM(shape, parts[0][0].dtype), [a for a, _ in parts])


def pick_half(block, half):
    n = block.shape[0] // 2

    def kernel(ref, out_ref):
        out_ref[...] = ref[pl.ds(half * n, n), :]

    return local_call(kernel, pltpu.VMEM((n, block.shape[1]), block.dtype), [block])


def join_halves(upper, lower):
    n = upper.shape[0]

    return local_call(join_kernel, pltpu.VMEM((2 * n, upper.shape[1]), upper.dtype), [upper, lower])


def place(stack, parts):
    def kernel(*refs):
        refs = refs if stack is None else refs[1:]
        z, c = lax.axis_index("z"), lax.axis_index("c")
        back = 1 - 2 * c
        for ref, (step, flip, _, index) in zip(refs, parts):
            core = 1 - c if flip else c
            at = lax.rem(z + back * step + NZ, NZ) * NC + core
            refs[-1][at, pl.ds(0, n), :] = block_of(ref, index)

    args = [a for _, _, a, _ in parts]
    n = args[0].shape[-1]
    out = pltpu.VMEM((NZ * NC, n + EXTRA, n), args[0].dtype)
    if stack is None:
        return local_call(kernel, out, args)
    return local_call(kernel, out, [stack, *args], aliases={0: 0})


def multiply(rows_ref, acc_ref, out_ref, parts, col_refs):
    x, y, c = (lax.axis_index(a) for a in ("x", "y", "c"))
    first = jnp.where(c == 0, x, y)
    second = jnp.where(c == 0, y, x)
    ats = []
    for j, i, _, _ in parts:
        p, q = lax.rem(first + 4 - j, 4), lax.rem(second + 4 - i, 4)
        ats.append(jnp.where(c == 0, p * NY + q, q * NY + p))
    half = out_ref.shape[1] // 2
    for band in (pl.ds(0, half), pl.ds(half, half + EXTRA)):
        total = None if acc_ref is None else acc_ref[band, :]
        for at, ref, (_, _, _, index) in zip(ats, col_refs, parts):
            part = jnp.dot(
                rows_ref[at, band, :], block_of(ref, index), preferred_element_type=jnp.float32
            )
            total = part if total is None else total + part
        out_ref[band, :] = total


def matmul_early(rows, parts):
    n = rows.shape[2]

    def kernel(rows_ref, *refs):
        multiply(rows_ref, None, refs[-1], parts, refs[:-1])

    return local_call(
        kernel,
        pltpu.VMEM((n + EXTRA, n), jnp.float32),
        [rows, *(a for _, _, a, _ in parts)],
        flops=2 * n * n * n * len(parts),
        limit=16,
    )


def matmul_late(rows, parts, product, keep_mask, thr_index, order_all):
    n = rows.shape[2]
    tiles = n // TB

    def kernel(keep_ref, thr_ref, rows_ref, *refs):
        col_refs, (acc_ref, out_ref, sums_ref) = refs[: len(parts)], refs[len(parts) :]
        multiply(rows_ref, acc_ref, out_ref, parts, col_refs)
        means = jnp.sum(out_ref[pl.ds(n, 8), :], axis=0, keepdims=True) / order_all
        cut = 0.125 * thr_ref[...].astype(jnp.float32) * means
        for j in range(tiles):
            cols = slice(j * TB, (j + 1) * TB)
            total = jnp.zeros((1, TB), jnp.float32)
            for i in range(tiles):
                at = (slice(i * TB, (i + 1) * TB), cols)
                keep = keep_ref[i, j].astype(jnp.float32)
                pruned = jnp.maximum(out_ref[at] - cut[:, cols], 0.0) * keep
                out_ref[at] = pruned
                total += jnp.sum(pruned, axis=0, keepdims=True)
            sums_ref[:, cols] = jnp.broadcast_to(total, (sums_ref.shape[0], TB))

    args = [keep_mask, thr_index, rows, *(a for _, _, a, _ in parts), product]
    return local_call(
        kernel,
        [pltpu.VMEM((n + EXTRA, n), jnp.float32), pltpu.VMEM((NX * NY, n), jnp.float32)],
        args,
        spaces=[SMEM] + [VMEM] * (len(args) - 1),
        aliases={len(args) - 1: 0},
        flops=2 * n * n * n * len(parts),
        limit=16,
    )


def expand_and_prune(values, tile_mask, keep_mask, thr_index):
    n = values.shape[0]
    order_all = n * NX * NY
    one = pltpu.VMEM((1, n), jnp.float32)
    own, own_sums = local_call(
        mask_kernel,
        [pltpu.VMEM((n, n), values.dtype), one],
        [tile_mask, values],
        [HBM] * 2,
        scratch=[
            pltpu.SMEM(tile_mask.shape, tile_mask.dtype),
            pltpu.VMEM(values.shape, values.dtype),
            pltpu.SemaphoreType.DMA((2,)),
        ],
    )

    other = partner(own)
    n1 = along_first(own, 1)
    n3 = along_first(own, -1)
    a1 = ring_z(own)
    up_o = along_second(own, 1)
    dn_o = along_second(own, -1)
    b1 = ring_z(other)
    a2 = ring_z(a1)
    b2 = ring_z(b1)
    a3 = ring_z(a2)
    b3 = ring_z(b2)
    a4 = ring_z(a3)
    n2_upper = along_first(pick_half(n1, 0), 1)
    n2_lower = along_first(pick_half(n3, 1), -1)
    pair = pack([(n1, None), (n3, None)])
    up_pair = along_second(pair, 1)
    dn_pair = along_second(pair, -1)
    n2 = join_halves(n2_upper, n2_lower)
    up_n2 = along_second(n2, 1)
    dn_n2 = along_second(n2, -1)
    far_a = along_second(pack([(up_o, None), (up_pair, 0)]), 1)
    far_n3 = along_second(pack([(dn_pair, 1)]), -1)
    far_n2 = along_second(dn_n2, -1)
    d1 = partner(pack([(a1, None), (b1, None)]))
    d2 = partner(pack([(a2, None), (b2, None)]))
    d3 = partner(pack([(a3, None), (b3, None)]))

    across = first_apart(own_sums, 2)
    sums = local_call(first_axis_kernel, one, [own_sums, across, n1, n3])
    sums = partner(sums)
    sums = local_call(add_kernel, one, [sums, first_apart(sums, 1)])
    sums = local_call(add_kernel, one, [sums, first_apart(sums, 2)])
    here = local_call(stack_kernel, pltpu.VMEM((2, n), jnp.float32), [partner(sums), sums])
    next_z = against_z(here, 1)
    before = partner(next_z)
    near = local_call(stack_kernel, pltpu.VMEM((6, n), jnp.float32), [here, next_z, before])
    ahead = against_z(near, 3)
    behind = partner(ahead)
    d4 = partner(a4)

    stack = pltpu.VMEM((NZ * NC, n + EXTRA, n), own.dtype)
    rows = place(None, [(0, False, own, None), (0, True, other, None)])
    rows = place(rows, [(-1, False, a1, None), (-1, True, b1, None)])
    rows = place(rows, [(-2, False, a2, None), (-2, True, b2, None)])
    rows = local_call(place_near_kernel, stack, [rows, near], aliases={0: 0})
    rows = place(rows, [(1, True, d1, 0), (1, False, d1, 1)])
    rows = place(rows, [(2, True, d2, 0), (2, False, d2, 1)])
    rows = local_call(place_far_kernel, stack, [rows, ahead, behind], aliases={0: 0})
    rows = place(rows, [(-3, False, a3, None), (-3, True, b3, None)])
    rows = place(rows, [(3, True, d3, 0), (3, False, d3, 1)])
    rows = place(rows, [(4, False, a4, None), (4, True, d4, None)])
    product = matmul_early(
        rows,
        [
            (0, 0, own, None), (1, 0, n1, None), (3, 0, n3, None), (2, 0, n2, None),
            (0, 1, up_o, None), (1, 1, up_pair, 0), (3, 1, up_pair, 1), (2, 1, up_n2, None),
            (0, 3, dn_o, None), (1, 3, dn_pair, 0), (3, 3, dn_pair, 1), (2, 3, dn_n2, None),
        ],
    )
    pruned, sums = matmul_late(
        rows,
        [(0, 2, far_a, 0), (1, 2, far_a, 1), (3, 2, far_n3, None), (2, 2, far_n2, None)],
        product,
        keep_mask,
        thr_index[None, :],
        order_all,
    )
    got = spread_over(sums, ROW)
    return local_call(
        functools.partial(scale_kernel, order_all),
        jax.ShapeDtypeStruct((n, n), values.dtype),
        [got, pruned],
    )


def solution(mesh):
    finer = Mesh(mesh.devices.reshape(NX, NY, NZ, NC), ("x", "y", "z", "c"))
    placed = (P(ROW, COL), P(ROW, COL), P(ROW, COL), P(COL))
    return jax.shard_map(
        expand_and_prune, mesh=finer, in_specs=placed, out_specs=P(ROW, COL), check_vma=False
    )
```

```python
import functools

import jax
import jax.numpy as jnp
from jax import lax
from jax.experimental import pallas as pl
from jax.experimental.pallas import tpu as pltpu
from jax.sharding import Mesh
from jax.sharding import PartitionSpec as P


TB = 128
EXTRA = 16
NX, NY, NZ, NC = 4, 4, 8, 2
ROW = ("x", "y")
COL = ("z", "c")

XYC = [(x, y, c) for x in range(NX) for y in range(NY) for c in range(NC)]
VMEM = pl.BlockSpec(memory_space=pltpu.VMEM)
HBM = pl.BlockSpec(memory_space=pltpu.HBM)
SMEM = pl.BlockSpec(memory_space=pltpu.SMEM)


def xyc(x, y, c):
    return ((x % NX) * NY + y % NY) * NC + c


def along_first(block, step):
    pairs = [(xyc(x, y, c), xyc(x + step, y, c) if c == 0 else xyc(x, y + step, c)) for x, y, c in XYC]
    return lax.ppermute(block, ("x", "y", "c"), pairs)


def along_second(block, step):
    pairs = [(xyc(x, y, c), xyc(x, y + step, c) if c == 0 else xyc(x + step, y, c)) for x, y, c in XYC]
    return lax.ppermute(block, ("x", "y", "c"), pairs)


def ring_z(block):
    pairs = [
        (z * NC + c, ((z + 1 - 2 * c) % NZ) * NC + c) for z in range(NZ) for c in range(NC)
    ]
    return lax.ppermute(block, ("z", "c"), pairs)


def first_apart(block, apart):
    pairs = [(xyc(x, y, c), xyc(x ^ apart, y, c) if c == 0 else xyc(x, y ^ apart, c)) for x, y, c in XYC]
    return lax.ppermute(block, ("x", "y", "c"), pairs)


def against_z(block, step):
    pairs = [
        (z * NC + c, ((z - step * (1 - 2 * c)) % NZ) * NC + c) for z in range(NZ) for c in range(NC)
    ]
    return lax.ppermute(block, ("z", "c"), pairs)


def partner(block):
    return lax.ppermute(block, "c", [(0, 1), (1, 0)])


def spread_over(rows, axes):
    return lax.all_to_all(rows, axes, 0, 0, tiled=True)


def kept_in(x, spec):
    if spec is SMEM:
        return x
    return pltpu.with_memory_space_constraint(x, spec.memory_space)


def local_call(
    kernel, out_shape, args, spaces=None, aliases=None, flops=0, limit=4, scratch=(),
    out_space=VMEM,
):
    spaces = spaces or [VMEM] * len(args)
    args = [kept_in(a, s) for a, s in zip(args, spaces)]
    return pl.pallas_call(
        kernel,
        out_shape=out_shape,
        in_specs=spaces,
        out_specs=jax.tree.map(lambda _: out_space, out_shape),
        scratch_shapes=scratch,
        input_output_aliases=aliases or {},
        cost_estimate=pl.CostEstimate(flops=flops, bytes_accessed=0, transcendentals=0),
        compiler_params=pltpu.CompilerParams(vmem_limit_bytes=limit << 20),
    )(*args)


def mask_kernel(mask_hbm, values_hbm, out_ref, sums_ref, mask_ref, values_ref, sems):
    fetch_mask = pltpu.make_async_copy(mask_hbm, mask_ref, sems.at[0])
    fetch_values = pltpu.make_async_copy(values_hbm, values_ref, sems.at[1])
    fetch_mask.start()
    fetch_values.start()
    fetch_mask.wait()
    fetch_values.wait()
    tiles = out_ref.shape[0] // TB
    for j in range(tiles):
        cols = slice(j * TB, (j + 1) * TB)
        total = jnp.zeros((1, TB), jnp.float32)
        for i in range(tiles):
            at = (slice(i * TB, (i + 1) * TB), cols)
            block = values_ref[at].astype(jnp.float32) * mask_ref[i, j].astype(jnp.float32)
            out_ref[at] = block.astype(out_ref.dtype)
            total += jnp.sum(block, axis=0, keepdims=True)
        sums_ref[:, cols] = total


def join_kernel(upper_ref, lower_ref, out_ref):
    n = upper_ref.shape[0]
    out_ref[pl.ds(0, n), :] = upper_ref[...]
    out_ref[pl.ds(n, n), :] = lower_ref[...]


def three_parts(exact):
    high = exact.astype(jnp.bfloat16).astype(jnp.float32)
    rest = exact - high
    mid = rest.astype(jnp.bfloat16).astype(jnp.float32)
    return high, mid, rest - mid


def place_sums(out_ref, sums, where):
    n = sums.shape[1]
    z, c = lax.axis_index("z"), lax.axis_index("c")
    row = lax.broadcasted_iota(jnp.int32, (EXTRA, n), 0)
    for i, (step, same) in enumerate(where):
        core = c if same else 1 - c
        at = lax.rem(z + (1 - 2 * c) * step + NZ, NZ) * NC + core
        high, mid, low = three_parts(sums[i : i + 1])
        parts = jnp.where(row == 0, high, jnp.where(row == 1, mid, jnp.where(row == 2, low, 0.0)))
        out_ref[at, pl.ds(n, EXTRA), :] = parts.astype(out_ref.dtype)


NEAR = ((0, True), (0, False), (1, True), (1, False), (-1, False), (-1, True))
AHEAD = tuple((3 + step, same) for step, same in NEAR)
BEHIND = tuple((-step, not same) for step, same in AHEAD)


def place_near_kernel(_, sums_ref, out_ref):
    place_sums(out_ref, sums_ref[...], NEAR)


def place_far_kernel(_, ahead_ref, behind_ref, out_ref):
    place_sums(out_ref, ahead_ref[...], AHEAD)
    place_sums(out_ref, behind_ref[...], BEHIND)


def first_axis_kernel(mine_ref, across_ref, n1_ref, n3_ref, out_ref):
    total = mine_ref[...] + across_ref[...]
    for ref in (n1_ref, n3_ref):
        total += jnp.sum(ref[...].astype(jnp.float32), axis=0, keepdims=True)
    out_ref[...] = total


def add_kernel(a_ref, b_ref, out_ref):
    out_ref[...] = a_ref[...] + b_ref[...]


def stack_kernel(*refs):
    at = 0
    for ref in refs[:-1]:
        refs[-1][pl.ds(at, ref.shape[0]), :] = ref[...]
        at += ref.shape[0]


def scale_kernel(order_all, got_ref, pruned_ref, out_hbm, out_ref, sems):
    totals = jnp.sum(got_ref[...], axis=0, keepdims=True) / order_all
    scale = 1.0 / jnp.maximum(totals, 0.1)
    copies = []
    for i in range(out_ref.shape[0] // TB):
        band = pl.ds(i * TB, TB)
        out_ref[band, :] = (pruned_ref[band, :] * scale).astype(out_ref.dtype)
        copies.append(pltpu.make_async_copy(out_ref.at[band, :], out_hbm.at[band, :], sems.at[i]))
        copies[-1].start()
    for copy in copies:
        copy.wait()


def block_of(ref, index):
    return ref[...] if index is None else ref[index]


def pack(parts):
    def kernel(*refs):
        for i, (_, index) in enumerate(parts):
            if len(parts) == 1:
                refs[-1][...] = block_of(refs[i], index)
            else:
                refs[-1][i] = block_of(refs[i], index)

    shape = parts[0][0].shape[-2:]
    shape = shape if len(parts) == 1 else (len(parts), *shape)
    return local_call(kernel, pltpu.VMEM(shape, parts[0][0].dtype), [a for a, _ in parts])


def pick_half(block, half):
    n = block.shape[0] // 2

    def kernel(ref, out_ref):
        out_ref[...] = ref[pl.ds(half * n, n), :]

    return local_call(kernel, pltpu.VMEM((n, block.shape[1]), block.dtype), [block])


def join_halves(upper, lower):
    n = upper.shape[0]

    return local_call(join_kernel, pltpu.VMEM((2 * n, upper.shape[1]), upper.dtype), [upper, lower])


def place(stack, parts):
    def kernel(*refs):
        refs = refs if stack is None else refs[1:]
        z, c = lax.axis_index("z"), lax.axis_index("c")
        back = 1 - 2 * c
        for ref, (step, flip, _, index) in zip(refs, parts):
            core = 1 - c if flip else c
            at = lax.rem(z + back * step + NZ, NZ) * NC + core
            refs[-1][at, pl.ds(0, n), :] = block_of(ref, index)

    args = [a for _, _, a, _ in parts]
    n = args[0].shape[-1]
    out = pltpu.VMEM((NZ * NC, n + EXTRA, n), args[0].dtype)
    if stack is None:
        return local_call(kernel, out, args)
    return local_call(kernel, out, [stack, *args], aliases={0: 0})


def multiply(rows_ref, acc_ref, out_ref, parts, col_refs):
    x, y, c = (lax.axis_index(a) for a in ("x", "y", "c"))
    first = jnp.where(c == 0, x, y)
    second = jnp.where(c == 0, y, x)
    ats = []
    for j, i, _, _ in parts:
        p, q = lax.rem(first + 4 - j, 4), lax.rem(second + 4 - i, 4)
        ats.append(jnp.where(c == 0, p * NY + q, q * NY + p))
    half = out_ref.shape[1] // 2
    for band in (pl.ds(0, half), pl.ds(half, half + EXTRA)):
        total = None if acc_ref is None else acc_ref[band, :]
        for at, ref, (_, _, _, index) in zip(ats, col_refs, parts):
            part = jnp.dot(
                rows_ref[at, band, :], block_of(ref, index), preferred_element_type=jnp.float32
            )
            total = part if total is None else total + part
        out_ref[band, :] = total


def matmul_early(rows, parts):
    n = rows.shape[2]

    def kernel(rows_ref, *refs):
        multiply(rows_ref, None, refs[-1], parts, refs[:-1])

    return local_call(
        kernel,
        pltpu.VMEM((n + EXTRA, n), jnp.float32),
        [rows, *(a for _, _, a, _ in parts)],
        flops=2 * n * n * n * len(parts),
        limit=16,
    )


def matmul_late(rows, parts, product, keep_mask, thr_index, order_all):
    n = rows.shape[2]
    tiles = n // TB

    def kernel(keep_ref, thr_ref, rows_ref, *refs):
        col_refs, (acc_ref, out_ref, sums_ref) = refs[: len(parts)], refs[len(parts) :]
        multiply(rows_ref, acc_ref, out_ref, parts, col_refs)
        means = jnp.sum(out_ref[pl.ds(n, 8), :], axis=0, keepdims=True) / order_all
        cut = 0.125 * thr_ref[...].astype(jnp.float32) * means
        for j in range(tiles):
            cols = slice(j * TB, (j + 1) * TB)
            total = jnp.zeros((8, TB), jnp.float32)
            for i in range(tiles):
                at = (slice(i * TB, (i + 1) * TB), cols)
                keep = keep_ref[i, j].astype(jnp.float32)
                pruned = jnp.maximum(out_ref[at] - cut[:, cols], 0.0) * keep
                out_ref[at] = pruned
                total += jnp.sum(pruned.reshape(TB // 8, 8, TB), axis=0)
            total = jnp.sum(total, axis=0, keepdims=True)
            sums_ref[:, cols] = jnp.broadcast_to(total, (sums_ref.shape[0], TB))

    args = [keep_mask, thr_index, rows, *(a for _, _, a, _ in parts), product]
    return local_call(
        kernel,
        [pltpu.VMEM((n + EXTRA, n), jnp.float32), pltpu.VMEM((NX * NY, n), jnp.float32)],
        args,
        spaces=[SMEM] + [VMEM] * (len(args) - 1),
        aliases={len(args) - 1: 0},
        flops=2 * n * n * n * len(parts),
        limit=16,
    )


def expand_and_prune(values, tile_mask, keep_mask, thr_index):
    n = values.shape[0]
    order_all = n * NX * NY
    one = pltpu.VMEM((1, n), jnp.float32)
    own, own_sums = local_call(
        mask_kernel,
        [pltpu.VMEM((n, n), values.dtype), one],
        [tile_mask, values],
        [HBM] * 2,
        scratch=[
            pltpu.SMEM(tile_mask.shape, tile_mask.dtype),
            pltpu.VMEM(values.shape, values.dtype),
            pltpu.SemaphoreType.DMA((2,)),
        ],
    )

    other = partner(own)
    n1 = along_first(own, 1)
    n3 = along_first(own, -1)
    a1 = ring_z(own)
    up_o = along_second(own, 1)
    dn_o = along_second(own, -1)
    b1 = ring_z(other)
    a2 = ring_z(a1)
    b2 = ring_z(b1)
    a3 = ring_z(a2)
    b3 = ring_z(b2)
    a4 = ring_z(a3)
    n2_upper = along_first(pick_half(n1, 0), 1)
    n2_lower = along_first(pick_half(n3, 1), -1)
    pair = pack([(n1, None), (n3, None)])
    up_pair = along_second(pair, 1)
    dn_pair = along_second(pair, -1)
    n2 = join_halves(n2_upper, n2_lower)
    up_n2 = along_second(n2, 1)
    dn_n2 = along_second(n2, -1)
    far_a = along_second(pack([(up_o, None), (up_pair, 0)]), 1)
    far_n3 = along_second(pack([(dn_pair, 1)]), -1)
    far_n2 = along_second(dn_n2, -1)
    d1 = partner(pack([(a1, None), (b1, None)]))
    d2 = partner(pack([(a2, None), (b2, None)]))
    d3 = partner(pack([(a3, None), (b3, None)]))

    across = first_apart(own_sums, 2)
    sums = local_call(first_axis_kernel, one, [own_sums, across, n1, n3])
    sums = partner(sums)
    sums = local_call(add_kernel, one, [sums, first_apart(sums, 1)])
    sums = local_call(add_kernel, one, [sums, first_apart(sums, 2)])
    here = local_call(stack_kernel, pltpu.VMEM((2, n), jnp.float32), [partner(sums), sums])
    next_z = against_z(here, 1)
    before = partner(next_z)
    near = local_call(stack_kernel, pltpu.VMEM((6, n), jnp.float32), [here, next_z, before])
    ahead = against_z(near, 3)
    behind = partner(ahead)
    d4 = partner(a4)

    stack = pltpu.VMEM((NZ * NC, n + EXTRA, n), own.dtype)
    rows = place(None, [(0, False, own, None), (0, True, other, None)])
    rows = place(rows, [(-1, False, a1, None), (-1, True, b1, None)])
    rows = place(rows, [(-2, False, a2, None), (-2, True, b2, None)])
    rows = local_call(place_near_kernel, stack, [rows, near], aliases={0: 0})
    rows = place(rows, [(1, True, d1, 0), (1, False, d1, 1)])
    rows = place(rows, [(2, True, d2, 0), (2, False, d2, 1)])
    rows = local_call(place_far_kernel, stack, [rows, ahead, behind], aliases={0: 0})
    rows = place(rows, [(-3, False, a3, None), (-3, True, b3, None)])
    rows = place(rows, [(3, True, d3, 0), (3, False, d3, 1)])
    rows = place(rows, [(4, False, a4, None), (4, True, d4, None)])
    product = matmul_early(
        rows,
        [
            (0, 0, own, None), (1, 0, n1, None), (3, 0, n3, None), (2, 0, n2, None),
            (0, 1, up_o, None), (1, 1, up_pair, 0), (3, 1, up_pair, 1), (2, 1, up_n2, None),
            (0, 3, dn_o, None), (1, 3, dn_pair, 0), (3, 3, dn_pair, 1), (2, 3, dn_n2, None),
        ],
    )
    pruned, sums = matmul_late(
        rows,
        [(0, 2, far_a, 0), (1, 2, far_a, 1), (3, 2, far_n3, None), (2, 2, far_n2, None)],
        product,
        keep_mask,
        thr_index[None, :],
        order_all,
    )
    got = spread_over(sums, ROW)
    return local_call(
        functools.partial(scale_kernel, order_all),
        jax.ShapeDtypeStruct((n, n), values.dtype),
        [got, pruned],
        out_space=HBM,
        scratch=[pltpu.VMEM((n, n), values.dtype), pltpu.SemaphoreType.DMA((n // TB,))],
    )


def solution(mesh):
    finer = Mesh(mesh.devices.reshape(NX, NY, NZ, NC), ("x", "y", "z", "c"))
    placed = (P(ROW, COL), P(ROW, COL), P(ROW, COL), P(COL))
    return jax.shard_map(
        expand_and_prune, mesh=finer, in_specs=placed, out_specs=P(ROW, COL), check_vma=False
    )
```
